32 devices in a mesh: seq: 8 (over z, x), rows: 4 (over y, core).
Axes of the slice: x: 2, y: 2, z: 4, core: 2. Of those that a mesh axis runs over, the one named last changes fastest.
Arguments:
- attn_in: bfloat16 [8192, 8192], P(('seq', 'rows')), may hold values from -6 to 6
- attn_out: bfloat16 [8192, 8192], P(('seq', 'rows')), may hold values from -6 to 6
- valid: int32 [8192], P(('seq', 'rows')), may hold values 0 or 1
- w_qkv: bfloat16 [10240, 8192], P('rows', 'seq'), may hold values from -6 to 6
- w_out: bfloat16 [8192, 8192], P('rows', 'seq'), may hold values from -6 to 6
- qkv_ranks: int32 [10240], P('rows'), may hold values from 3072 to 5120
- out_ranks: int32 [8192], P('rows'), may hold values from 3072 to 5120
Outputs:
- qkv_margins: float32 [10240, 8192], P('rows', 'seq')
- out_margins: float32 [8192, 8192], P('rows', 'seq')
The draws below stay inside these ranges and needn't reach their ends.
Inputs may be any that keep to these rules, and one draw needn't show every extreme that they name: `qkv_ranks`: each row keeps between three and five eighths of its 8192 weights. `out_ranks`: each row keeps between three and five eighths of its 8192 weights.
All inputs are finite; a program needn't handle non-finite values. No bound on the sum of `valid` on one device may be relied on, other than what follows from the above.
Results may differ from the reference program's by a relative error of at most 0.0003.
Values may be sent and summed in bfloat16 or wider, within the bound.
A program may use at most 128 MiB of HBM per device.

```python
import jax
import jax.numpy as jnp
from jax import lax

D = 8192
QKV = 10240
TOK_DEV = 256
TOKENS = 8192


def with_ends(values, stream_key, least, largest):
    spot = [jax.random.randint(jax.random.fold_in(stream_key, axis), (), 0, length) for axis, length in enumerate(values.shape)]
    main_axis = values.shape.index(max(values.shape))
    beside = spot[:main_axis] + [(spot[main_axis] + 1) % values.shape[main_axis]] + spot[main_axis + 1:]
    return values.at[tuple(spot)].set(least).at[tuple(beside)].set(largest)


def raised(array, key, source, target, blocks, factor):
    owner, partner = [(jnp.arange(array.shape[axis_at]) // (array.shape[axis_at] // blocks)).reshape([-1 if axis == axis_at else 1 for axis in range(array.ndim)]) for axis_at in (source, target)]
    chosen = jax.random.permutation(key, blocks)[partner]
    strong = (owner == chosen) | (owner == (partner + blocks // 2) % blocks)
    return jnp.where(strong, factor * array, array)


def block_levels(key, dims, cuts, smallest, largest):
    gain = 1.0
    for dim, shards_of in cuts:
        steps = jax.random.uniform(jax.random.fold_in(jax.random.fold_in(key, 6), dim), (shards_of,), jnp.float32, smallest / len(cuts), largest / len(cuts))
        gain = gain * jnp.repeat(jnp.exp(steps), dims[dim] // shards_of).reshape((-1,) + (1,) * (len(dims) - 1 - dim))
    return gain


def bell_draw(key, extent, spread, reach, cuts=(), held_as=jnp.bfloat16):
    gain = block_levels(key, extent, cuts, -0.22, 0.18) if cuts else 1.0
    array = jax.random.normal(key, extent, jnp.float32) * spread * gain
    return jnp.minimum(jnp.maximum(array, -reach), reach).astype(held_as)


def noise_with(rng, shape, scale, most, cuts, heavy, kind=jnp.bfloat16):
    drawn = scale * jax.random.normal(rng, shape, jnp.float32)
    if cuts:
        drawn = drawn * block_levels(rng, shape, cuts, -0.22, 0.18)
    return jnp.clip(raised(drawn, jax.random.fold_in(rng, 3), *heavy), -most, most).astype(kind)


def setup_inputs(seed: int = 0) -> dict:
    keys = jax.random.split(jax.random.key(seed), 8)
    return {
        "attn_in": noise_with(keys[0], (TOKENS, D), 1.0, 6.0, ((0, 32),), (0, 1, 32, 2.75)),
        "attn_out": noise_with(keys[1], (TOKENS, D), 1.0, 6.0, ((0, 32),), (0, 1, 32, 2.75)),
        "valid": with_ends((jax.random.randint(keys[2], (TOKENS,), 0, 4) < 3).astype(jnp.int32), jax.random.fold_in(keys[2], 1), 0, 1),
        "w_qkv": bell_draw(keys[3], (QKV, D), 1.0, 6.0, ((0, 4), (1, 8))),
        "w_out": bell_draw(keys[4], (D, D), 1.0, 6.0, ((0, 4), (1, 8))),
        "qkv_ranks": with_ends(jax.random.randint(keys[5], (QKV,), 3 * D // 8, 5 * D // 8 + 1), jax.random.fold_in(keys[5], 1), 3 * D // 8, (5 * D // 8 + 1) - 1).astype(jnp.int32),
        "out_ranks": with_ends(jax.random.randint(keys[6], (D,), 3 * D // 8, 5 * D // 8 + 1), jax.random.fold_in(keys[6], 1), 3 * D // 8, (5 * D // 8 + 1) - 1).astype(jnp.int32),
    }


EPS = 1e-06

def column_norm(acts, valid):
    blocks = acts.reshape(TOKENS // TOK_DEV, TOK_DEV, D)
    marks = valid.reshape(TOKENS // TOK_DEV, TOK_DEV)

    def step(carry, item):
        rows, flags = item
        rows32 = rows.astype(jnp.float32)
        weight = flags.astype(jnp.float32)[:, None]
        return (carry + lax.optimization_barrier(jnp.sum(rows32 * rows32 * weight, axis=0)), None)
    total, unused = lax.scan(step, jnp.zeros((D,), jnp.float32), (blocks, marks))
    return jnp.sqrt(total / TOKENS + EPS)

def row_margins(weights, norm, ranks):
    scores = jnp.abs(weights.astype(jnp.float32)) * norm[None, :]
    ordered = -jnp.sort(-scores, axis=1)
    position = lax.broadcasted_iota(jnp.int32, ordered.shape, 1)
    chosen = (ranks.astype(jnp.int32) - 1)[:, None]
    limit = lax.optimization_barrier(jnp.sum(jnp.where(position == chosen, ordered, 0.0), axis=1))
    return jnp.maximum(scores - limit[:, None], 0.0)

def blocked(weights, norm, ranks):
    count = weights.shape[0]
    wblocks = weights.reshape(count // 128, 128, weights.shape[1])
    rblocks = ranks.reshape(count // 128, 128)
    result = lax.map(lambda item: row_margins(item[0], norm, item[1]), (wblocks, rblocks))
    return result.reshape(count, weights.shape[1])

def reference(attn_in, attn_out, valid, w_qkv, w_out, qkv_ranks, out_ranks):
    in_norm = column_norm(attn_in, valid)
    out_norm = column_norm(attn_out, valid)
    return (blocked(w_qkv, in_norm, qkv_ranks), blocked(w_out, out_norm, out_ranks))
```

```python
import functools

import jax
import jax.numpy as jnp
from jax import lax
from jax.experimental import pallas as pl
from jax.experimental.pallas import tpu as pltpu
from jax.sharding import PartitionSpec as P

EPS = 1e-06
LANES = 128
BIG = 3.0e38
MESH = pl.DeviceIdType.MESH
PLAN = ((4, 0.06, 0.0), (4, 3.5, 1.0), (4, 3.0, 1.0), (4, 2.0, 1.0),
        (4, None, 0.0), (4, None, 0.0), (4, None, 0.0))


def search_kernel(
    n_seq, n_rows, cols, tokens, groups, *refs
):
    (part_ref, wq_ref, wo_ref, kq_ref, ko_ref,
     norm_ref, loq_ref, hiq_ref, loo_ref, hio_ref, flag_ref,
     scores, normb, precv, psum, rrecv, probes, entries,
     sendq, sendo, recvq, recvo, flag_mine, flag_recv,
     p_send, p_recv, r_send, r_recv, q_send, q_recv, o_send, o_recv,
     f_send, f_recv) = refs
    me = lax.axis_index("seq")
    my_row = lax.axis_index("rows")
    width = cols * n_seq
    blocks = cols // LANES
    base = float(1 << cols.bit_length())
    w_refs = (wq_ref, wo_ref)
    k_refs = (kq_ref, ko_ref)
    sends = (sendq, sendo)
    recvs = (recvq, recvo)
    s_sems = (q_send, o_send)
    r_sems = (q_recv, o_recv)
    starts = (0, groups[0])
    rounds = len(PLAN)

    def seq_peer(offset):
        return lax.rem(me + offset, n_seq)

    def row_peer(offset):
        return lax.rem(my_row + offset, n_rows)

    barrier = pltpu.get_barrier_semaphore()
    for offset in range(1, n_seq):
        pl.semaphore_signal(barrier, inc=1, device_id={"seq": seq_peer(offset)}, device_id_type=MESH)
    for offset in range(1, n_rows):
        pl.semaphore_signal(barrier, inc=1, device_id={"rows": row_peer(offset)}, device_id_type=MESH)
    pl.semaphore_wait(barrier, n_seq + n_rows - 2)

    def start_all(axis, count, peer_of, mine, source_of, landing, ssem_of, rsem_of):
        copies = []
        for offset in range(1, count):
            peer = peer_of(offset)
            copy = pltpu.make_async_remote_copy(
                src_ref=source_of(peer), dst_ref=landing(mine),
                send_sem=ssem_of(offset), recv_sem=rsem_of(mine),
                device_id={axis: peer}, device_id_type=MESH)
            copy.start()
            copies.append(copy)
        return copies

    def wait_all(axis, count, peer_of, source_of, landing, ssem_of, rsem_of):
        for offset in range(1, count):
            peer = peer_of(offset)
            pltpu.make_async_remote_copy(
                src_ref=source_of(peer), dst_ref=landing(peer),
                send_sem=ssem_of(offset), recv_sem=rsem_of(peer),
                device_id={axis: peer}, device_id_type=MESH).wait_recv()

    pending = []
    p_args = (lambda peer: part_ref.at[peer], lambda slot: precv.at[slot],
              lambda o: p_send.at[o], lambda s: p_recv.at[s])
    pending += start_all("seq", n_seq, seq_peer, me, *p_args)
    precv[me] = part_ref[me]

    for half in range(2):
        def flip(step, carry, half=half):
            g = step // blocks
            c = step % blocks
            row = pl.multiple_of(g * LANES, LANES)
            col = pl.multiple_of(c * LANES, LANES)
            block = w_refs[half][pl.ds(row, LANES), pl.ds(col, LANES)].astype(jnp.float32)
            scores[starts[half] + g, pl.ds(col, LANES), :] = jnp.abs(block).T
            return carry
        lax.fori_loop(0, groups[half] * blocks, flip, 0, unroll=4)

    wait_all("seq", n_seq, seq_peer, *p_args)
    total = precv[0]
    for s in range(1, n_seq):
        total = total + precv[s]
    psum[...] = total
    rrecv[my_row] = total
    r_args = (lambda peer: psum, lambda slot: rrecv.at[slot],
              lambda o: r_send.at[o], lambda s: r_recv.at[s])
    pending += start_all("rows", n_rows, row_peer, my_row, *r_args)
    wait_all("rows", n_rows, row_peer, *r_args)
    total = rrecv[0]
    for s in range(1, n_rows):
        total = total + rrecv[s]
    norm = jnp.sqrt(total / tokens + EPS)
    norm_ref[...] = norm
    for i in range(2 * blocks):
        normb[i] = jnp.broadcast_to(norm[i:i + 1, :], (LANES, LANES)).T

    def fold(values):
        return values.reshape(LANES // 8, 8, LANES)

    def round_args(half, r, words):
        def part(ref):
            return ref.at[pl.ds(0, words)]
        return (lambda peer: part(sends[half].at[r]),
                lambda slot: part(recvs[half].at[r, slot]),
                lambda o: s_sems[half].at[r, o],
                lambda s: r_sems[half].at[r, s])

    def publish(half, r, words):
        out = []
        for w in range(words):
            recvs[half][r, me, w] = sends[half][r, w]
        out = start_all("seq", n_seq, seq_peer, me, *round_args(half, r, words))
        pending.extend(out)

    def collect(half, r, words):
        wait_all("seq", n_seq, seq_peer, *round_args(half, r, words))

    for half in range(2):
        def scale(g, carry, half=half):
            def column(c, acc):
                col = pl.multiple_of(c * LANES, LANES)
                value = scores[starts[half] + g, pl.ds(col, LANES), :] * normb[half * blocks + c]
                scores[starts[half] + g, pl.ds(col, LANES), :] = value
                return acc + jnp.sum(fold(value), axis=0)
            acc = lax.fori_loop(0, blocks, column, jnp.zeros((8, LANES), jnp.float32), unroll=True)
            sends[half][0, 0, pl.ds(g, 1), :] = jnp.sum(acc, axis=0, keepdims=True)
            return carry
        lax.fori_loop(0, groups[half], scale, 0)
        publish(half, 0, 1)

    state = [None, None]

    def spread(half, r):
        count, wide, extra = PLAN[r]
        guess, lo, hi, clo, chi, k = state[half]
        steps = [i - (count - 1) / 2 for i in range(count)]
        if r == 0:
            points = [guess * (1.0 + s * wide * 1.2) for s in steps]
        elif wide is None:
            top = jnp.where(hi > 1.0e38, 2.0 * lo + guess, hi)
            points = [lo + (top - lo) * (0.5 + s / (count + 1)) for s in steps]
        else:
            top = jnp.where(hi > 1.0e38, 2.0 * lo + guess, hi)
            below = clo - k + 0.5
            above = k - 0.5 - chi
            inside = jnp.maximum(clo - chi, 1.0)
            deviation = wide * jnp.sqrt(jnp.maximum(below * above / inside, 0.0)) + extra
            points = [lo + (top - lo) * jnp.clip((below + s * deviation) / inside, 0.02, 0.98)
                      for s in steps]
        for i in range(1, count):
            points[i] = jnp.maximum(points[i], points[i - 1])
        for i in range(count):
            probes[half, i, pl.ds(0, groups[half]), :] = points[i]
        return points

    def count_all(half, r):
        count = PLAN[r][0]
        def group(g, carry):
            limits = [jnp.broadcast_to(probes[half, i, pl.ds(g, 1), :], (LANES, LANES))
                      for i in range(count)]
            def column(c, accs):
                col = pl.multiple_of(c * LANES, LANES)
                value = scores[starts[half] + g, pl.ds(col, LANES), :]
                out = []
                for w in range(count // 2):
                    marked = jnp.where(value >= limits[2 * w + 1], base + 1.0,
                                       jnp.where(value >= limits[2 * w], 1.0, 0.0))
                    out.append(accs[w] + jnp.sum(fold(marked), axis=0))
                return tuple(out)
            zero = jnp.zeros((8, LANES), jnp.float32)
            accs = lax.fori_loop(0, blocks, column, (zero,) * (count // 2), unroll=2)
            for w in range(count // 2):
                sends[half][r + 1, w, pl.ds(g, 1), :] = jnp.sum(accs[w], axis=0, keepdims=True)
            return carry
        lax.fori_loop(0, groups[half], group, 0)

    def narrow(half, r, points):
        count = PLAN[r][0]
        guess, lo, hi, clo, chi, k = state[half]
        for w in range(count // 2):
            lower = jnp.zeros_like(lo)
            upper = jnp.zeros_like(lo)
            for s in range(n_seq):
                word = recvs[half][r + 1, s, w]
                high = jnp.floor(word * (1.0 / base))
                upper = upper + high
                lower = lower + (word - high * base)
            for point, number in ((points[2 * w], lower), (points[2 * w + 1], upper)):
                enough = number >= k
                rise = enough & (point > lo)
                fall = (number < k) & (point < hi)
                lo = jnp.where(rise, point, lo)
                clo = jnp.where(rise, number, clo)
                hi = jnp.where(fall, point, hi)
                chi = jnp.where(fall, number, chi)
        state[half] = (guess, lo, hi, clo, chi, k)

    points = [None, None]
    for r in range(rounds):
        for half in range(2):
            if r == 0:
                collect(half, 0, 1)
                sums = recvs[half][0, 0, 0]
                for s in range(1, n_seq):
                    sums = sums + recvs[half][0, s, 0]
                mean = sums * (1.0 / width)
                k = k_refs[half][...]
                p = k * (1.0 / width) - 0.5
                guess = mean * (0.845 - 1.996 * p + 1.12 * p * p)
                zero = jnp.zeros_like(k)
                state[half] = (guess, zero, zero + BIG, zero + float(width), zero, k)
            else:
                collect(half, r, PLAN[r - 1][0] // 2)
                narrow(half, r - 1, points[half])
            points[half] = spread(half, r)
            count_all(half, r)
            publish(half, r + 1, PLAN[r][0] // 2)

    last = rounds + 1
    for half in range(2):
        collect(half, rounds, PLAN[-1][0] // 2)
        narrow(half, rounds - 1, points[half])
        guess, lo, hi, clo, chi, k = state[half]
        probes[half, 0, pl.ds(0, groups[half]), :] = lo
        probes[half, 1, pl.ds(0, groups[half]), :] = hi
        def ends(g, carry, half=half):
            low = jnp.broadcast_to(probes[half, 0, pl.ds(g, 1), :], (LANES, LANES))
            high = jnp.broadcast_to(probes[half, 1, pl.ds(g, 1), :], (LANES, LANES))
            def column(c, accs):
                col = pl.multiple_of(c * LANES, LANES)
                value = scores[starts[half] + g, pl.ds(col, LANES), :]
                least = jnp.min(fold(jnp.where(value >= low, value, BIG)), axis=0)
                most = jnp.max(fold(jnp.where(value < high, value, -1.0)), axis=0)
                return (jnp.minimum(accs[0], least), jnp.maximum(accs[1], most))
            least, most = lax.fori_loop(
                0, blocks, column,
                (jnp.full((8, LANES), BIG, jnp.float32), jnp.full((8, LANES), -1.0, jnp.float32)),
                unroll=2)
            sends[half][last, 0, pl.ds(g, 1), :] = jnp.min(least, axis=0, keepdims=True)
            sends[half][last, 1, pl.ds(g, 1), :] = jnp.max(most, axis=0, keepdims=True)
            return carry
        lax.fori_loop(0, groups[half], ends, 0)
        publish(half, last, 2)

    open_rows = jnp.zeros((1, LANES), jnp.float32)
    for half in range(2):
        collect(half, last, 2)
        guess, lo, hi, clo, chi, k = state[half]
        span = pl.ds(0, groups[half])
        known = jnp.zeros_like(lo)
        least_all = jnp.full_like(lo, BIG)
        most_all = jnp.full_like(lo, -1.0)
        for s in range(n_seq):
            least = recvs[half][last, s, 0]
            most = recvs[half][last, s, 1]
            least_all = jnp.minimum(least_all, least)
            most_all = jnp.maximum(most_all, most)
            has = least < hi
            two = has & (most > least)
            entries[half, 2 * s, span, :] = jnp.where(has, least, BIG)
            entries[half, 2 * s + 1, span, :] = jnp.where(two, most, BIG)
            known = known + jnp.where(has, 1.0, 0.0) + jnp.where(two, 1.0, 0.0)
        place = clo - k

        def pick(e, found):
            mine = entries[half, e, span, :]
            less = jnp.zeros_like(mine)
            upto = jnp.zeros_like(mine)
            for other in range(2 * n_seq):
                value = entries[half, other, span, :]
                less = less + jnp.where(value < mine, 1.0, 0.0)
                upto = upto + jnp.where(value <= mine, 1.0, 0.0)
            hit = (less <= place) & (upto > place) & (mine < BIG)
            return jnp.where(hit, mine, found)

        found = lax.fori_loop(0, 2 * n_seq, pick, jnp.full_like(lo, -1.0))
        whole = (known == clo - chi) & (found >= 0.0)
        first = clo == k
        final = chi == k - 1.0
        limit = jnp.where(first, least_all, jnp.where(final, most_all, found))
        solved = first | final | whole
        lo_ref, hi_ref = ((loq_ref, hiq_ref), (loo_ref, hio_ref))[half]
        lo_ref[...] = jnp.where(solved, limit, lo)
        hi_ref[...] = jnp.where(solved, limit, hi)
        open_rows = open_rows + jnp.sum(jnp.where(solved, 0.0, 1.0), axis=0, keepdims=True)

    flag_mine[...] = jnp.broadcast_to(open_rows, (8, LANES))
    flag_recv[my_row] = flag_mine[...]
    f_args = (lambda peer: flag_mine, lambda slot: flag_recv.at[slot],
              lambda o: f_send.at[o], lambda s: f_recv.at[s])
    pending += start_all("rows", n_rows, row_peer, my_row, *f_args)
    wait_all("rows", n_rows, row_peer, *f_args)
    total = flag_recv[0]
    for s in range(1, n_rows):
        total = total + flag_recv[s]
    flag_ref[...] = total
    for copy in pending:
        copy.wait_send()


def per_device(attn_in, attn_out, valid, w_qkv, w_out, qkv_ranks, out_ranks):
    n_seq, n_rows = lax.axis_size("seq"), lax.axis_size("rows")
    weight = valid.astype(jnp.float32)[:, None]

    def squares(acts):
        acts32 = acts.astype(jnp.float32)
        return jnp.sum(acts32 * acts32 * weight, axis=0)

    tokens = attn_in.shape[0] * n_seq * n_rows
    cols = w_qkv.shape[1]
    blocks = cols // LANES
    partial = jnp.stack([squares(attn_in), squares(attn_out)])
    partial = partial.reshape(2, n_seq, blocks, LANES).transpose(1, 0, 2, 3)
    partial = partial.reshape(n_seq, 2 * blocks, LANES)
    groups = (w_qkv.shape[0] // LANES, w_out.shape[0] // LANES)
    ranks = [r.astype(jnp.float32).reshape(-1, LANES) for r in (qkv_ranks, out_ranks)]
    steps = len(PLAN) + 2
    most = max(groups)
    vmem = pl.BlockSpec(memory_space=pltpu.VMEM)
    f32 = jnp.float32

    def shape(*dims):
        return jax.ShapeDtypeStruct(dims, f32)

    dma = pltpu.SemaphoreType.DMA
    norm, loq, hiq, loo, hio, flag = pl.pallas_call(
        functools.partial(search_kernel, n_seq, n_rows, cols, tokens, groups),
        out_shape=[shape(2 * blocks, LANES), shape(groups[0], LANES), shape(groups[0], LANES),
                   shape(groups[1], LANES), shape(groups[1], LANES), shape(8, LANES)],
        in_specs=[vmem] * 5,
        out_specs=[vmem] * 6,
        scratch_shapes=[
            pltpu.VMEM((sum(groups), cols, LANES), f32),
            pltpu.VMEM((2 * blocks, LANES, LANES), f32),
            pltpu.VMEM((n_seq, 2 * blocks, LANES), f32),
            pltpu.VMEM((2 * blocks, LANES), f32),
            pltpu.VMEM((n_rows, 2 * blocks, LANES), f32),
            pltpu.VMEM((2, 4, most, LANES), f32),
            pltpu.VMEM((2, 2 * n_seq, most, LANES), f32),
            pltpu.VMEM((steps, 2, groups[0], LANES), f32),
            pltpu.VMEM((steps, 2, groups[1], LANES), f32),
            pltpu.VMEM((steps, n_seq, 2, groups[0], LANES), f32),
            pltpu.VMEM((steps, n_seq, 2, groups[1], LANES), f32),
            pltpu.VMEM((8, LANES), f32),
            pltpu.VMEM((n_rows, 8, LANES), f32),
            dma((n_seq,)), dma((n_seq,)), dma((n_rows,)), dma((n_rows,)),
            dma((steps, n_seq)), dma((steps, n_seq)), dma((steps, n_seq)), dma((steps, n_seq)),
            dma((n_rows,)), dma((n_rows,)),
        ],
        compiler_params=pltpu.CompilerParams(
            collective_id=0, has_side_effects=True, vmem_limit_bytes=60 * 1024 * 1024),
        name="search",
    )(partial, w_qkv, w_out, *ranks)
    norm = norm.reshape(2, cols)

    def scored(weights, row):
        return jnp.abs(weights.astype(f32)) * norm[row][None, :]

    def going(state):
        return state[0] > 0.0

    def halve(state):
        unused, bounds = state
        results = []
        active = jnp.float32(0.0)
        for row, (weights, ranked) in enumerate(((w_qkv, qkv_ranks), (w_out, out_ranks))):
            low, high = bounds[2 * row], bounds[2 * row + 1]
            middle = 0.5 * (low + high)
            counted = jnp.sum((scored(weights, row) >= middle[:, None]).astype(f32), axis=1)
            counted = lax.psum(counted, "seq")
            rising = counted >= ranked.astype(f32)
            moving = (middle > low) & (middle < high)
            results.append(jnp.where(moving & rising, middle, low))
            results.append(jnp.where(moving & ~rising, middle, high))
            active = jnp.maximum(active, jnp.max(moving.astype(f32)))
        return (lax.psum(active, ("seq", "rows")), tuple(results))

    start = (flag[0].sum(), tuple(x.reshape(-1) for x in (loq, hiq, loo, hio)))
    unused, bounds = lax.while_loop(going, halve, start)
    return (
        jnp.maximum(scored(w_qkv, 0) - bounds[0][:, None], 0.0),
        jnp.maximum(scored(w_out, 1) - bounds[2][:, None], 0.0),
    )


def solution(mesh):
    placed = (
        P(("seq", "rows"), None),
        P(("seq", "rows"), None),
        P(("seq", "rows")),
        P("rows", "seq"),
        P("rows", "seq"),
        P("rows"),
        P("rows"),
    )
    return jax.shard_map(
        per_device,
        mesh=mesh,
        in_specs=placed,
        out_specs=(P("rows", "seq"), P("rows", "seq")),
        check_vma=False,
    )
```
